32 devices in a mesh: leaf: 16 (over z, y, x), sep: 2 (over core).
Axes of the slice: x: 2, y: 2, z: 4, core: 2. Of those that a mesh axis runs over, the one named last changes fastest.
Arguments:
- leaf_rhs: bfloat16 [16, 256, 2048], P('leaf', None, 'sep'), may hold values from -6 to 6
- leaf_inv: bfloat16 [16, 2048, 2048], P('leaf', 'sep'), may hold values from -0.125 to 0.125
- leaf_couple: bfloat16 [16, 512, 2048], P('leaf', None, 'sep'), may hold values from -0.0625 to 0.0625
- sep_rhs: float32 [16, 256, 512], P('leaf', None, 'sep'), may hold values from -6 to 6
- sep_inv: float32 [16, 512, 512], P('leaf', 'sep'), may hold values from -0.25 to 0.25
- sep_couple: float32 [16, 512, 512], P('leaf', None, 'sep'), may hold values from -0.1875 to 0.1875
Outputs:
- leaf_solution: float32 [16, 256, 2048], P('leaf', None, 'sep')
- sep_solution: float32 [16, 256, 512], P('leaf', None, 'sep')
The draws below stay inside these ranges and needn't reach their ends.
All inputs are finite; a program needn't handle non-finite values.
Results may differ from the reference program's by a relative error of at most 0.0042.
Values may be sent and summed in bfloat16 or wider, within the bound.
A program may use at most 128 MiB of HBM per device.

```python
import jax
import jax.numpy as jnp
import numpy as np
from jax import lax

NI = 2048
S = 512
RHS = 256
LEAVES = 16
LEVELS = 4


def levels(key, extent, shards, smallest, high):
    factor_of = 1.0
    for axis_at, parts in shards:
        steps = jax.random.uniform(jax.random.fold_in(jax.random.fold_in(key, 6), axis_at), (parts,), jnp.float32, smallest / len(shards), high / len(shards))
        factor_of = factor_of * jnp.repeat(jnp.exp(steps), extent[axis_at] // parts).reshape((-1,) + (1,) * (len(extent) - 1 - axis_at))
    return factor_of


def gaussian(key, shape, deviation, most, shards=(), held_as=jnp.bfloat16):
    result = jax.random.normal(key, shape, jnp.float32) * deviation
    if len(shards) > 0:
        result = levels(key, shape, shards, -0.22, 0.18) * result
    return jnp.clip(result, min=-most, max=most).astype(held_as)


def setup_inputs(seed: int = 0) -> dict:
    arg_keys = jax.random.split(jax.random.key(seed), 7)
    return {
        "leaf_rhs": gaussian(arg_keys[0], (LEAVES, RHS, NI), 1.0, 6.0, ((0, 16), (2, 2))),
        "leaf_inv": gaussian(arg_keys[1], (LEAVES, NI, NI), NI ** -0.5, 0.125, ((0, 16), (1, 2))),
        "leaf_couple": gaussian(arg_keys[2], (LEAVES, S, NI), (4 * NI) ** -0.5, 0.0625, ((0, 16), (2, 2))),
        "sep_rhs": gaussian(arg_keys[3], (LEAVES, RHS, S), 1.0, 6.0, ((0, 16), (2, 2)), jnp.float32),
        "sep_inv": gaussian(arg_keys[4], (LEAVES, S, S), S ** -0.5, 0.25, ((0, 16), (1, 2)), jnp.float32),
        "sep_couple": gaussian(arg_keys[5], (LEAVES, S, S), (2 * S) ** -0.5, 0.1875, ((0, 16), (2, 2)), jnp.float32),
    }


def leaf_up(items):
    rhs, inverse, couple = items
    dims = (((1,), (1,)), ((), ()))
    state = lax.dot_general(rhs, inverse, dims, preferred_element_type=jnp.float32).astype(jnp.bfloat16)
    return state, lax.dot_general(state, couple, dims, preferred_element_type=jnp.float32)


def leaf_down(items):
    state, parent, couple, inverse = items
    pulled = jnp.dot(parent.astype(jnp.bfloat16), couple, preferred_element_type=jnp.float32)
    residue = (state.astype(jnp.float32) - pulled).astype(jnp.bfloat16)
    return jnp.dot(residue, inverse, preferred_element_type=jnp.float32)


def reference(leaf_rhs, leaf_inv, leaf_couple, sep_rhs, sep_inv, sep_couple):
    count = leaf_rhs.shape[0]
    high = lax.Precision.HIGHEST
    leaf_state, leaf_out = lax.map(leaf_up, (leaf_rhs, leaf_inv, leaf_couple))
    sep_state = jnp.zeros(sep_rhs.shape, jnp.float32)
    outgoing = leaf_out
    for section in range(1, LEVELS + 2):
        slots = np.arange(2 ** (section - 1) - 1, count, 2 ** section)
        if section == 1:
            children = outgoing[slots] + outgoing[slots + 1]
        elif section <= LEVELS:
            reach = 2 ** (section - 2)
            children = outgoing[slots - reach] + outgoing[slots + reach]
        else:
            children = outgoing[slots - 2 ** (section - 2)]
        work = sep_rhs[slots] - children
        fresh = jnp.einsum("brk,bmk->brm", work, sep_inv[slots], precision=high)
        sep_state = sep_state.at[slots].set(fresh)
        if section <= LEVELS:
            sent = jnp.einsum("brk,bmk->brm", fresh, sep_couple[slots], precision=high)
            outgoing = jnp.zeros(sep_rhs.shape, jnp.float32).at[slots].set(sent)
    sep_solution = jnp.zeros(sep_rhs.shape, jnp.float32)
    for section in range(LEVELS + 1, 0, -1):
        slots = np.arange(2 ** (section - 1) - 1, count, 2 ** section)
        if section == LEVELS + 1:
            work = sep_state[slots]
        else:
            reach = 2 ** (section - 1)
            parent = np.where(((slots >> section) & 1) == 0, slots + reach, slots - reach)
            work = sep_state[slots] - jnp.einsum("brk,bkm->brm", sep_solution[parent], sep_couple[slots], precision=high)
        solved = jnp.einsum("brk,bkm->brm", work, sep_inv[slots], precision=high)
        sep_solution = sep_solution.at[slots].set(solved)
    numbers = np.arange(count)
    parents = numbers - numbers % 2
    leaf_solution = lax.map(leaf_down, (leaf_state, sep_solution[parents], leaf_couple, leaf_inv))
    return leaf_solution, sep_solution
```

```python
import functools

import jax
import jax.numpy as jnp
from jax import lax
from jax.experimental import pallas as pl
from jax.experimental.pallas import tpu as pltpu
from jax.sharding import PartitionSpec as P

F32 = jnp.float32
BF16 = jnp.bfloat16
CHUNKS = 4
RECEIVES = 68


def dot_nt(a, b):
    return lax.dot_general(a, b, (((1,), (1,)), ((), ())), preferred_element_type=F32)


def dot_nn(a, b):
    return lax.dot_general(a, b, (((1,), (0,)), ((), ())), preferred_element_type=F32)


def dot_tn(a, b):
    return lax.dot_general(a, b, (((0,), (0,)), ((), ())), preferred_element_type=F32)


def halves(value):
    high = value.astype(BF16)
    return high, (value - high.astype(F32)).astype(BF16)


def three_pass(a, b, dot):
    ah, al = halves(a)
    bh, bl = halves(b)
    return dot(ah, bh) + (dot(ah, bl) + dot(al, bh))


def two_pass(a, b, dot):
    rows = a.shape[0]
    both = dot(jnp.concatenate(halves(a), axis=0), b)
    return both[:rows] + both[rows:]


def scope(name):
    return jax.named_scope(name)


def kernel(
    leaves,
    rhs_hbm, inv_hbm, couple_hbm, srhs_hbm, sinv_hbm, scpl_hbm,
    leaf_out, sep_out,
    rhs, inv, couple, srhs, sinv, scpl, other_rhs, state,
    parts, part_in, fac, top, srows, rb, rp, rt,
    out_send, out_own, out_in, base, xs, xr, w1s, o1, ys, yr,
    zb, zr, w2s, w3s, w4s, sols, sb, dn, w1g, sg, s2, s3, s4, st,
    fin_s, fin_r, sep_acc,
    load_sem, send_sem, recv_sem,
):
    p = lax.axis_index("leaf")
    c = lax.axis_index("sep")
    oc = 1 - c
    b0 = p % 2
    b1 = (p // 2) % 2
    q = p // 4
    place = p % 4
    planes = leaves // 4
    below_top = planes // 2 - 1
    xp = p + 1 - 2 * b0
    yp = p + 2 - 4 * b1
    mate = (p, oc)
    rows = rhs.shape[0]
    part = rhs.shape[1]
    width = sinv.shape[1]
    half = width // 2
    mid = rows // 2
    quarter = rows // 4
    eighth = rows // 8
    chunk = half // CHUNKS

    left, right = b0 == 0, b0 == 1
    near, far = b1 == 0, b1 == 1
    even_plane = q % 2 == 0
    odd_plane = jnp.logical_not(even_plane)
    last = q == planes - 1
    joint = q == below_top
    is_top = p == leaves - 1
    node = odd_plane & jnp.logical_not(last)
    fourth = q % 4 == 1
    pair_plane = q + 1 - 2 * (q % 2)
    reach = 1
    for bit in range(leaves.bit_length()):
        reach = jnp.where((q + 1) % (2 ** (bit + 1)) == 0, 2 ** (bit + 1), reach)
    upper = (q // (2 * reach)) % 2 == 1
    parent = jnp.where(upper, q - reach, q + reach)
    low_child = q - reach // 2
    high_child = q + reach // 2
    climbs = node & jnp.logical_not(joint)
    inner = node & jnp.logical_not(fourth)

    def over(plane):
        return (4 * plane + place, c)

    def in_plane(dc, dx, dy):
        return (4 * q + 2 * ((b1 + dy) % 2) + (b0 + dx) % 2, (c + dc) % 2)

    def when(cond, action):
        if cond is None:
            action()
        else:
            @pl.when(cond)
            def _():
                action()

    others = [(dc, dx, dy) for dx in range(2) for dy in range(2) for dc in range(2) if (dc, dx, dy) != (0, 0, 0)]
    peers = [(None, in_plane(*other)) for other in others] + [
        (None, over(pair_plane)),
        (fourth, over(q + 1)),
        (q % 4 == 2, over(q - 1)),
        (fourth, over(q + 2)),
        (q % 4 == 3, over(q - 2)),
        (climbs, over(parent)),
        (inner, over(low_child)),
        (inner, over(high_child)),
        (last, over(below_top)),
        (joint, over(planes - 1)),
    ]
    barrier = pltpu.get_barrier_semaphore()
    expected = 0
    for cond, to in peers:
        when(cond, lambda to=to: pl.semaphore_signal(barrier, inc=1, device_id=to, device_id_type=pl.DeviceIdType.MESH))
        expected = expected + (1 if cond is None else jnp.where(cond, 1, 0))

    own_cols = pl.ds(pl.multiple_of(c * part, part), part)
    other_cols = pl.ds(pl.multiple_of(oc * part, part), part)
    loads = []
    for src, dst in (
        (sinv_hbm.at[0], sinv),
        (scpl_hbm.at[0], scpl),
        (rhs_hbm.at[0], rhs),
        (srhs_hbm.at[0], srhs),
        (inv_hbm.at[0, :, own_cols], inv.at[:, own_cols]),
        (inv_hbm.at[0, :, other_cols], inv.at[:, other_cols]),
        (couple_hbm.at[0], couple),
    ):
        copy = pltpu.make_async_copy(src, dst, load_sem.at[len(loads)])
        copy.start()
        loads.append(copy)

    pending = []
    names = {}

    def sem(*name):
        return recv_sem.at[names.setdefault(name, len(names))]

    def remote(src, dst, rsem, to):
        return pltpu.make_async_remote_copy(
            src_ref=src, dst_ref=dst, send_sem=send_sem.at[0], recv_sem=rsem,
            device_id=to, device_id_type=pl.DeviceIdType.MESH,
        )

    def push(src, dst, rsem, to, cond=None):
        copy = remote(src, dst, rsem, to)
        when(cond, lambda: copy.start())
        pending.append((cond, copy))

    def arrive(dst, rsem, cond=None):
        copy = remote(dst, dst, rsem, mate)
        when(cond, lambda: copy.wait_recv())

    loads[0].wait()
    loads[1].wait()

    @pl.when(is_top)
    def _():
        parts[0] = three_pass(sinv[...], sinv[...], dot_tn).reshape(2, half, width)

    @pl.when(jnp.logical_not(is_top))
    def _():
        parts[0] = three_pass(scpl[...], sinv[...], dot_nn).reshape(2, half, width)

    loads[2].wait()
    loads[3].wait()
    with scope("barrier"):
        pl.semaphore_wait(barrier, expected)

    push(parts.at[0, oc], part_in.at[0], sem("part", 0), mate)
    push(rhs, other_rhs, sem("rhs"), mate)

    for k in range(2):
        for h in range(2):
            sem("rb", k, h)
    for dc, dx, dy in others:
        to = in_plane(dc, dx, dy)
        block = to[1] * 4 + (to[0] % 4) % 2 * 2 + (to[0] % 4) // 2
        push(
            srhs.at[pl.ds(pl.multiple_of(block * eighth, eighth), eighth)], rb.at[b1, c],
            recv_sem.at[names[("rb", 0, 0)] + 2 * b1 + c], to, right,
        )
    block8 = c * 4 + b0 * 2 + b1

    @pl.when(right)
    def _():
        rb[b1, c] = srhs[pl.ds(pl.multiple_of(block8 * eighth, eighth), eighth), :]

    push(srhs.at[pl.ds(pl.multiple_of(oc * mid, mid), mid)], srows.at[c], sem("srows"), mate, left)

    @pl.when(left)
    def _():
        srows[c] = srhs[pl.ds(pl.multiple_of(c * mid, mid), mid), :]

    parts[1] = three_pass(sinv[...], sinv[...], dot_tn).reshape(2, half, width)
    push(parts.at[1, oc], part_in.at[1], sem("part", 1), mate)

    loads[4].wait()
    piece = part // 4
    for j in range(4):
        at_j = pl.ds(j * piece, piece)
        leaf_out[:, at_j] = dot_nt(rhs[...], inv[at_j, own_cols])

    own = b0 * (1 + b1)
    theirs = (1 - b0) * (1 + b1)
    across = 2 - b1
    paired = 2 + q % 2

    def spot(kind, idx, core, i):
        return fac.at[kind, idx, core, pl.ds(i * chunk, chunk)]

    def share_up(kind, idx, i, cond):
        push(spot(kind, idx, c, i), spot(kind, 3, c, i), sem("z", kind, i // 2), over(pair_plane), even_plane & cond)
        if kind == 0:
            push(
                spot(kind, idx, c, i), top.at[c, pl.ds(i * chunk, chunk)], sem("top"), over(below_top), last & cond,
            )

    def own_x(kind, chunks, cond=None):
        for i in chunks:
            push(spot(kind, own, c, i), spot(kind, own, c, i), sem("x", kind, i), (xp, c), cond)

    def own_y(kind, chunks):
        for i in chunks:
            push(spot(kind, own, c, i), spot(kind, own, c, i), sem("y", kind, i), (yp, c), right)
            share_up(kind, own, i, right & far)

    def own_mate(kind):
        push(fac.at[kind, own, c], fac.at[kind, own, c], sem("own", kind), mate)

    def relay_x(kind, chunks=range(CHUNKS)):
        for i in chunks:
            arrive(spot(kind, theirs, c, i), sem("x", kind, i))
            push(spot(kind, theirs, c, i), spot(kind, theirs, c, i), sem("y", kind, i), (yp, c), left)
            push(spot(kind, theirs, c, i), spot(kind, theirs, c, i), sem("theirs", kind), mate)
            share_up(kind, theirs, i, left & far)

    def relay_y(kind, cond=None):
        for i in range(CHUNKS):
            arrive(spot(kind, across, c, i), sem("y", kind, i), cond)
            push(spot(kind, across, c, i), spot(kind, across, c, i), sem("across", kind), mate, cond)
            share_up(kind, across, i, near if cond is None else near & cond)

    def relay_z(kind):
        for k in range(2):
            span = pl.ds(k * half // 2, half // 2)
            arrive(fac.at[kind, 3, c, span], sem("z", kind, k), odd_plane)
            push(fac.at[kind, 3, c, span], fac.at[kind, 3, c, span], sem("paired", kind), mate, odd_plane)

    def whole(kind, which):
        idx = {"own": own, "theirs": theirs, "across": across, "paired": 3}[which]
        arrive(fac.at[kind, idx, oc], sem(which, kind), odd_plane if which == "paired" else None)

    def factor(kind, idx):
        return fac[kind, idx].reshape(width, width)

    with scope("part0"):
        arrive(part_in.at[0], sem("part", 0))
    fac[0, own, c] = (parts[0, c] + part_in[0]).astype(BF16)
    own_x(0, range(CHUNKS), left)
    own_x(0, range(CHUNKS - 1), right)
    own_y(0, range(CHUNKS))
    own_mate(0)

    with scope("rhs"):
        arrive(other_rhs, sem("rhs"))
    loads[5].wait()
    for j in range(4):
        at_j = pl.ds(j * piece, piece)
        state[:, at_j] = (leaf_out[:, at_j] + dot_nt(other_rhs[...], inv[at_j, other_cols])).astype(BF16)
    loads[6].wait()
    out_send[...] = dot_nt(state[pl.ds(pl.multiple_of(oc * mid, mid), mid), :], couple[...])
    push(out_send, out_in, sem("out"), mate)
    out_own[...] = dot_nt(state[pl.ds(pl.multiple_of(c * mid, mid), mid), :], couple[...])

    arrive(part_in.at[1], sem("part", 1))
    fac[1, own, c] = (parts[1, c] + part_in[1]).astype(BF16)
    own_mate(1)

    arrive(srows.at[oc], sem("srows"), left)
    with scope("out"):
        arrive(out_in, sem("out"))
    given = jnp.where(left, jnp.concatenate([srows[0], srows[1]], axis=1), 0.0)
    base[...] = (given - (out_own[...] + out_in[...])).reshape(2, quarter, width)
    xs[...] = base[1 - b0].astype(BF16)
    push(xs, xr, sem("xr"), (xp, c))
    own_x(0, range(CHUNKS - 1, CHUNKS), right)
    own_x(1, range(CHUNKS))
    own_y(1, range(2))

    with scope("relay_x0"):
        relay_x(0)
    with scope("relay_y0"):
        relay_y(0, right)
    with scope("xr"):
        arrive(xr, sem("xr"))
    with scope("m1"):
        whole(0, "own")
        whole(0, "theirs")
    w1s[...] = base[b0] + xr[...].astype(F32)
    o1[...] = two_pass(-w1s[...], factor(0, 0), dot_nt).reshape(2, eighth, width)
    ys[...] = o1[1 - b1].astype(BF16)
    push(ys, yr, sem("yr"), (yp, c))
    own_y(1, range(2, CHUNKS))
    with scope("relay_y0"):
        relay_y(0, left)

    for k in range(2):
        for h in range(2):
            arrive(rb.at[k, h], sem("rb", k, h), jnp.logical_not(right & (b1 == k) & (c == h)))
    push(rb.at[1], rp, sem("rp"), over(pair_plane), even_plane)
    push(rb.at[1], rt, sem("rt"), over(below_top), last)
    with scope("m2"):
        whole(0, "across")
    with scope("yr"):
        arrive(yr, sem("yr"))
    w2s[...] = jnp.concatenate([rb[0, 0], rb[0, 1]], axis=1) + (o1[b1] + yr[...].astype(F32))
    out2 = two_pass(w2s[...], factor(0, 1), dot_nt)
    zb[0] = out2.astype(BF16)
    zb_own = w3s
    zb_own[...] = out2
    push(zb.at[0], zr.at[0], sem("zr", 0), over(pair_plane))

    with scope("relay_z0"):
        relay_z(0)
    with scope("relay_x1"):
        relay_x(1)
    arrive(rp, sem("rp"), odd_plane)
    with scope("zr0"):
        arrive(zr.at[0], sem("zr", 0))
    with scope("m3"):
        whole(0, "paired")
    given = jnp.where(
        even_plane, jnp.concatenate([rb[1, 0], rb[1, 1]], axis=1), jnp.concatenate([rp[0], rp[1]], axis=1)
    )
    w3s[...] = given - (w3s[...] + zr[0].astype(F32))
    out3 = two_pass(w3s[...], factor(0, paired), dot_nt)
    zb[1] = out3.astype(BF16)
    st[...] = out3
    push(zb.at[1], zr.at[1], sem("zr", 1), over(q - 1), q % 4 == 2)

    with scope("relay_y1"):
        relay_y(1)

    sem("zr", 2)
    arrive(zr.at[2], sem("zr", 2), inner)
    with scope("zr1"):
        arrive(zr.at[1], sem("zr", 1), node)

    @pl.when(node)
    def _():
        first = jnp.where(fourth, st[...], zr[2].astype(F32))
        w4s[...] = jnp.concatenate([rb[1, 0], rb[1, 1]], axis=1) - (first + zr[1].astype(F32))
        out4 = two_pass(w4s[...], factor(0, 2), dot_nt)
        st[...] = out4
        zb[2] = out4.astype(BF16)

    up = jnp.where(upper, 1, 2)
    push(
        zb.at[2], zr.at[up], recv_sem.at[jnp.where(upper, names[("zr", 1)], names[("zr", 2)])], over(parent), climbs,
    )
    arrive(top.at[c], sem("top"), joint)
    push(top.at[c], top.at[c], sem("top_mate"), mate, joint)
    arrive(rt, sem("rt"), joint)
    with scope("n3"):
        for which in ("own", "theirs", "across"):
            whole(1, which)
    arrive(top.at[oc], sem("top_mate"), joint)

    @pl.when(joint)
    def _():
        wt = jnp.concatenate([rt[0], rt[1]], axis=1) - st[...]
        st[...] = two_pass(wt, top[...].reshape(width, width), dot_nn)

    with scope("dn1"):
        arrive(dn.at[1], sem("dn", 1), climbs)

    @pl.when(node)
    def _():
        above = jnp.where(joint, st[...], dn[1].astype(F32))
        s4[...] = two_pass(w4s[...], factor(1, 2), dot_nn) - two_pass(above, factor(0, 2), dot_nn)
        sb[...] = s4[...].astype(BF16)

    for plane in (q - 1, q + 1, q + 2):
        push(sb, dn.at[0], sem("dn", 0), over(plane), fourth)
    for plane in (low_child, high_child):
        push(sb, dn.at[1], sem("dn", 1), over(plane), inner)
    push(st, sols, sem("top_back"), over(planes - 1), joint)

    w1n = two_pass(w1s[...], factor(1, 0), dot_nn)
    slot = c * 2 + b0
    w1g[slot] = w1n.astype(BF16)
    for dc, dx in ((1, 0), (0, 1), (1, 1)):
        push(w1g.at[slot], w1g.at[slot], sem("w1n", dc, dx), in_plane(dc, dx, 0))
    w2s[...] = two_pass(w2s[...], factor(1, 1), dot_nn)
    with scope("relay_z1"):
        relay_z(1)
        whole(1, "paired")
    w3s[...] = two_pass(w3s[...], factor(1, paired), dot_nn)

    with scope("dn0"):
        arrive(dn.at[0], sem("dn", 0), jnp.logical_not(fourth))
    above3 = jnp.where(fourth, sb[...], dn[0])
    s3[...] = w3s[...] - dot_nn(above3, factor(0, paired))
    s2[...] = w2s[...] - dot_nn(s3[...].astype(BF16), factor(0, 1))
    sg[block8] = s2[...].astype(BF16)
    for dx, dy, dc in ((1, 0, 0), (0, 1, 0), (1, 0, 1), (0, 1, 1), (1, 1, 0), (1, 1, 1), (0, 0, 1)):
        push(sg.at[block8], sg.at[block8], sem("sg", dc, dx, dy), in_plane(dc, dx, dy))

    def deliver(src, to, cond):
        for h in range(2):
            cols = pl.ds(h * half, half)
            here = (p == to) & (c == h)
            push(src.at[:, cols], sep_acc.at[block8], sem("acc"), (to, h), cond & jnp.logical_not(here))

            @pl.when(here & cond)
            def _():
                sep_acc[block8] = src[:, cols]

    def backward(group, side):
        spans = [
            pl.ds(pl.multiple_of(t * quarter + side * eighth, eighth), eighth) for t in range(4)
        ]
        inside = pl.ds(pl.multiple_of(side * eighth, eighth), eighth)
        above = jnp.concatenate([sg[2 * t + side] for t in range(4)], axis=0)
        free = jnp.concatenate([w1g[t, inside] for t in range(4)], axis=0).astype(F32)
        sol1 = free - dot_nn(above, factor(0, 0))

        @pl.when(left)
        def _():
            mine = jnp.where(c == 0, sol1[:, :half], sol1[:, half:])
            for t in range(4):
                sep_out[spans[t], :] = mine[t * eighth:(t + 1) * eighth]

        before = jnp.concatenate([state[span, :] for span in spans], axis=0).astype(F32)
        residue = (before - dot_nn(sol1.astype(BF16), couple[...])).astype(BF16)
        for j in range(4):
            cols = pl.ds(pl.multiple_of(oc * part + j * piece, piece), piece)
            fin_s[group, j] = dot_nn(residue, inv[:, cols]).astype(BF16)
            push(fin_s.at[group, j], fin_r.at[group, j], sem("fin", group, j), mate)
        for j in range(4):
            cols = pl.ds(pl.multiple_of(c * part + j * piece, piece), piece)
            value = dot_nn(residue, inv[:, cols])
            for t in range(4):
                leaf_out[spans[t], pl.ds(j * piece, piece)] = value[t * eighth:(t + 1) * eighth]
        return spans

    def gathered(dc, dx, dy):
        block = ((c + dc) % 2) * 4 + ((b0 + dx) % 2) * 2 + (b1 + dy) % 2
        arrive(sg.at[block], sem("sg", dc, dx, dy))

    with scope("w1n"):
        for dc, dx in ((1, 0), (0, 1), (1, 1)):
            arrive(w1g.at[((c + dc) % 2) * 2 + (b0 + dx) % 2], sem("w1n", dc, dx))
    with scope("sg0"):
        gathered(1, 0, 0)
        gathered(0, 1, 0)
        gathered(1, 1, 0)
    spans = [backward(0, b1)]
    with scope("sg1"):
        for dc, dx in ((0, 0), (1, 0), (0, 1), (1, 1)):
            gathered(dc, dx, 1)
    always = q >= 0
    deliver(s2, 4 * q + 1, always)
    deliver(s3, 4 * q + 3, even_plane)
    deliver(s4, 4 * q + 3, node)
    arrive(sols, sem("top_back"), last)
    deliver(sols, 4 * q + 3, last)
    spans.append(backward(1, 1 - b1))
    with scope("fin"):
        for group in range(2):
            for j in range(4):
                arrive(fin_r.at[group, j], sem("fin", group, j))
                for t in range(4):
                    leaf_out[spans[group][t], pl.ds(j * piece, piece)] += fin_r[
                        group, j, pl.ds(t * eighth, eighth)
                    ].astype(F32)

    with scope("acc"):
        arrive(sep_acc.at[pl.ds(0, 7)], sem("acc"), right)

    @pl.when(right)
    def _():
        sep_out[...] = sep_acc[...].reshape(rows, half)

    with scope("drain"):
        for cond, copy in pending:
            when(cond, lambda copy=copy: copy.wait_send())
    assert len(names) == RECEIVES, len(names)


def local(leaves, leaf_rhs, leaf_inv, leaf_couple, sep_rhs, sep_inv, sep_couple):
    _, rows, part = leaf_rhs.shape
    full = leaf_inv.shape[2]
    width = sep_inv.shape[2]
    half = width // 2
    mid, quarter, eighth = rows // 2, rows // 4, rows // 8
    vmem = pl.BlockSpec(memory_space=pltpu.VMEM)
    anywhere = pl.BlockSpec(memory_space=pl.ANY)
    V = pltpu.VMEM
    dma = pltpu.SemaphoreType.DMA
    leaf_solution, sep_solution = pl.pallas_call(
        functools.partial(kernel, leaves),
        out_shape=(pltpu.VMEM((rows, part), F32), pltpu.VMEM((rows, half), F32)),
        in_specs=[anywhere] * 6,
        out_specs=(vmem, vmem),
        scratch_shapes=[
            V((rows, part), BF16), V((part, full), BF16), V((width, part), BF16), V((rows, half), F32),
            V((half, width), F32), V((width, half), F32), V((rows, part), BF16), V((rows, part), BF16),
            V((2, 2, half, width), F32), V((2, half, width), F32), V((2, 4, 2, half, width), BF16),
            V((2, half, width), BF16), V((2, mid, half), F32), V((2, 2, eighth, half), F32),
            V((2, eighth, half), F32), V((2, eighth, half), F32),
            V((mid, width), F32), V((mid, width), F32), V((mid, width), F32), V((2, quarter, width), F32),
            V((quarter, width), BF16), V((quarter, width), BF16), V((quarter, width), F32),
            V((2, eighth, width), F32), V((eighth, width), BF16), V((eighth, width), BF16),
            V((3, eighth, width), BF16), V((3, eighth, width), BF16), V((eighth, width), F32),
            V((eighth, width), F32), V((eighth, width), F32), V((eighth, width), F32), V((eighth, width), BF16),
            V((2, eighth, width), BF16), V((4, quarter, width), BF16), V((8, eighth, width), BF16),
            V((eighth, width), F32), V((eighth, width), F32), V((eighth, width), F32), V((eighth, width), F32),
            V((2, 4, mid, part // 4), BF16), V((2, 4, mid, part // 4), BF16), V((8, eighth, half), F32),
            dma((7,)), dma((1,)), dma((RECEIVES,)),
        ],
        compiler_params=pltpu.CompilerParams(
            collective_id=0, has_side_effects=True, vmem_limit_bytes=60 * 1024 * 1024
        ),
    )(leaf_rhs, leaf_inv, leaf_couple, sep_rhs, sep_inv, sep_couple)
    return leaf_solution[None], sep_solution[None]


def solution(mesh):
    return jax.shard_map(
        functools.partial(local, mesh.shape["leaf"]),
        mesh=mesh,
        in_specs=(
            P("leaf", None, "sep"),
            P("leaf", "sep", None),
            P("leaf", None, "sep"),
            P("leaf", None, "sep"),
            P("leaf", "sep", None),
            P("leaf", None, "sep"),
        ),
        out_specs=(P("leaf", None, "sep"), P("leaf", None, "sep")),
        check_vma=False,
    )
```
